32 devices in a mesh: dp: 8 (over z, core), expert: 4 (over y, x).
Axes of the slice: x: 2, y: 2, z: 4, core: 2. Of those that a mesh axis runs over, the one named last changes fastest.
Arguments:
- tokens: bfloat16 [16384, 2048], P(('dp', 'expert')), parts along dimension 0, may hold values from -6 to 6
- modality: int32 [16384], P(('dp', 'expert')), parts along dimension 0, may hold values 0 or 1
- expert_ids: int32 [16384, 2], P(('dp', 'expert')), parts along dimension 0, may hold values from 0 to 3, all different within a row; in each aligned block of 512 rows (0 to 511, 512 to 1023, ...) at most 320 rows name the same one
- route_weights: float32 [16384, 2], P(('dp', 'expert')), parts along dimension 0, may hold values from 0.25 to 1
- norm_gain: float32 [2, 2048], replicated, may hold values from 0.25 to 1.75
- gate_weight: bfloat16 [2048, 3584], P(None, 'expert'), may hold values from -0.125 to 0.125
- up_weight: bfloat16 [2048, 3584], P(None, 'expert'), may hold values from -0.125 to 0.125
- down_weight: bfloat16 [3584, 2048], P('expert'), may hold values from -0.1875 to 0.1875
Outputs:
- mixed: bfloat16 [16384, 2048], P(('dp', 'expert')), parts along dimension 0
The draws below stay inside these ranges and needn't reach their ends.
There are 8 independent parts, one for each index of `dp`. The reference program is written for one: setup_inputs(seed, part) draws one part's arguments, and reference() takes and returns one part's arrays. A program takes and returns all parts, laid end to end along the dimension named above; an argument that names none is the same for every part. Nothing has to cross between parts.
Inputs may be any that keep to these rules, and one draw needn't show every extreme that they name: `expert_ids`: each row names 2 different experts. Among the rows of one device no expert is named by more than 320 rows, a bound that some blocks reach.
All inputs are finite; a program needn't handle non-finite values. No bound on the sum of `modality` on one device may be relied on, other than what follows from the above.
Results may differ from the reference program's by a relative error of at most 0.0054.
Values may be sent and summed in bfloat16 or wider, within the bound.
A program may use at most 128 MiB of HBM per device.

```python
import math
import jax
import jax.numpy as jnp
import numpy as np
from jax import lax

D = 2048
HIDDEN_SIZE = 896
TOP = 2
TOK_DEV = 512
EXPERTS = 4
CAP = 320
TOKENS = 2048
N_EXPERT = 4


def set_ends(result, stream_key, low, largest):
    dims = result.shape
    index_at = [jax.random.randint(jax.random.fold_in(stream_key, axis), (), 0, dims[axis]) for axis in range(len(dims))]
    result = result.at[tuple(index_at)].set(low)
    longest = dims.index(max(dims))
    index_at[longest] = (index_at[longest] + 1) % dims[longest]
    return result.at[tuple(index_at)].set(largest)


def block_scale(own_key, shape, shards, least, high):
    def one(dim, shards_of):
        steps = jax.random.uniform(jax.random.fold_in(jax.random.fold_in(own_key, 6), dim), (shards_of,), jnp.float32, least / len(shards), high / len(shards))
        return jnp.repeat(jnp.exp(steps), shape[dim] // shards_of).reshape((-1,) + (1,) * (len(shape) - dim - 1))

    gain = one(*shards[0])
    for cut in shards[1:]:
        gain = gain * one(*cut)
    return gain


def deal_out(key, own, number, rows, count, top, limit, lean):
    order = jax.random.permutation(key, count)
    heavy_load, ordinary = shares(count, rows * top, limit, lean, True), shares(count, rows * top, limit, lean, False)
    places = jnp.arange(count)

    def named(sizes, offset_by):
        used = int((sizes > 0).sum())
        fixed = max(1, used // 4)
        moved = fixed + (places - fixed + offset_by * (used - fixed)) % max(1, count - fixed)
        return jnp.zeros((count,), jnp.int32).at[order[jnp.where(places < fixed, places, moved)]].set(jnp.asarray(sizes, jnp.int32))

    sizes = jnp.where(number % 4 == 0, named(heavy_load, number // 4), named(ordinary, number - number // 4 - 1))
    mixed = jax.random.permutation(jax.random.fold_in(own, 3), count)
    source_of, taker = mixed[0:count // 2 * 2:2], mixed[1:count // 2 * 2:2]
    room = jnp.minimum(sizes[source_of] - 1, limit - sizes[taker]) // 2
    room = jnp.where((source_of == order[0]) | (taker == order[0]) | (sizes[taker] == 0), 0, jnp.maximum(room, 0))
    moved = jax.random.randint(jax.random.fold_in(own, 4), (count // 2,), 0, 1 << 20) % (room + 1)
    sizes = sizes.at[source_of].add(-moved).at[taker].add(moved)
    labels = jnp.searchsorted(jnp.cumsum(sizes), jnp.arange(rows * top), side="right").astype(jnp.int32)
    table = labels.reshape(top, rows).T
    table = table[jax.random.permutation(jax.random.fold_in(own, 1), rows)]
    offset_by = jax.random.randint(jax.random.fold_in(own, 2), (rows, 1), 0, top)
    return jnp.take_along_axis(table, (jnp.arange(top)[None, :] + offset_by) % top, axis=1)


def shares(number_of, total, bound, slope, full):
    loads = [(1 << 20) // math.isqrt(rank ** slope) + 1 for rank in range(1, number_of + 1)]
    largest = bound if full else min(bound, max(-(-total // number_of), total * loads[0] // sum(loads)))
    least = 1 if total - largest >= number_of - 1 else 0
    counts, rest = [largest] + [least] * (number_of - 1), total - largest - least * (number_of - 1)
    while rest > 0:
        free = [i for i in range(1, number_of) if counts[i] < largest] or [i for i in range(1, number_of) if counts[i] < bound]
        pool, budget = sum([loads[i] for i in free]), rest
        for i in free:
            extra = min(bound - counts[i], max(1, budget * loads[i] // pool), rest)
            counts[i] = counts[i] + extra
            rest = rest - extra
    return np.array(counts)


def bell_draw(stream_key, shape, spread, most, split=(), held_as=jnp.bfloat16):
    factor_of = block_scale(stream_key, shape, split, -0.22, 0.18) if split else 1.0
    result = jax.random.normal(stream_key, shape, jnp.float32) * spread * factor_of
    return jnp.minimum(jnp.maximum(result, -most), most).astype(held_as)


def setup_inputs(seed: int = 0, part: int = 0) -> dict:
    key_list = jax.random.split(jax.random.key(seed), 9)
    part_splits = jax.random.split(jax.random.fold_in(key_list[8], part), 9)
    tokens = bell_draw(part_splits[0], (TOKENS, D), 1.0, 6.0, ((0, 4),))
    modality = set_ends((jax.random.randint(part_splits[1], (TOKENS,), 0, 2) < 1).astype(jnp.int32), jax.random.fold_in(part_splits[1], 1), 0, 1)
    expert_ids_keys = jax.random.split(jax.random.fold_in(part_splits[2], 1), TOKENS // TOK_DEV)
    expert_ids_turns = jax.random.permutation(jax.random.fold_in(part_splits[2], 3), TOKENS // TOK_DEV)
    expert_ids = jax.vmap(lambda own, number: deal_out(jax.random.fold_in(part_splits[2], 2), own, number, TOK_DEV, EXPERTS, TOP, CAP, 1))(expert_ids_keys, expert_ids_turns).reshape((TOKENS, TOP))
    route_weights = jnp.clip(0.25 + 0.75 * jax.random.uniform(part_splits[3], (TOKENS, TOP), jnp.float32) ** block_scale(part_splits[3], (TOKENS, TOP), ((0, 4),), -0.2, 0.2), 0.25, 1.0)
    norm_gain = jnp.clip(1.0 + 0.15 * jax.random.normal(key_list[4], (2, D), jnp.float32), 0.25, 1.75)
    gate_weight = bell_draw(key_list[5], (D, EXPERTS * HIDDEN_SIZE), D ** -0.5, 0.125, ((1, 4),))
    up_weight = bell_draw(key_list[6], (D, EXPERTS * HIDDEN_SIZE), D ** -0.5, 0.125, ((1, 4),))
    down_weight = bell_draw(key_list[7], (EXPERTS * HIDDEN_SIZE, D), HIDDEN_SIZE ** -0.5, 0.1875, ((0, 4),))
    return dict(tokens=tokens, modality=modality, expert_ids=expert_ids, route_weights=route_weights, norm_gain=norm_gain, gate_weight=gate_weight, up_weight=up_weight, down_weight=down_weight)


epsilon = 1e-05

def normalize(tokens, modality, norm_gain):
    values = tokens.astype(jnp.float32)
    square = lax.optimization_barrier(jnp.mean(values * values, axis=1, keepdims=True))
    gains = jnp.where(modality[:, None] == 1, norm_gain[1][None, :], norm_gain[0][None, :])
    return (values * lax.rsqrt(square + epsilon) * gains).astype(jnp.bfloat16)

def slot_table(expert_ids, experts, capacity):
    fanout = expert_ids.shape[1]
    flat_ids = expert_ids.reshape(-1).astype(jnp.int32)
    columns = jnp.arange(experts, dtype=jnp.int32)
    onehot = (flat_ids[:, None] == columns[None, :]).astype(jnp.int32)
    earlier = jnp.cumsum(onehot, axis=0).astype(jnp.int32) - onehot
    position = lax.optimization_barrier(jnp.sum(earlier * onehot, axis=1)).astype(jnp.int32)
    slots = (flat_ids * capacity + position).astype(jnp.int32)
    sources = (jnp.arange(flat_ids.shape[0], dtype=jnp.int32) // fanout).astype(jnp.int32)
    owners = jnp.full((experts * capacity,), -1, jnp.int32).at[slots].set(sources)
    return (slots, owners)

def pack_rows(normed, owners):
    chosen = jnp.take(normed, jnp.maximum(owners, 0), axis=0)
    return jnp.where(owners[:, None] >= 0, chosen, jnp.zeros_like(chosen))

def expert_rows(rows, gate_cols, up_cols, down_rows):
    gate = jnp.dot(rows, gate_cols, preferred_element_type=jnp.float32)
    upper = jnp.dot(rows, up_cols, preferred_element_type=jnp.float32)
    active = (jax.nn.silu(gate) * upper).astype(jnp.bfloat16)
    return jnp.dot(active, down_rows, preferred_element_type=jnp.float32)

def reference(tokens, modality, expert_ids, route_weights, norm_gain, gate_weight, up_weight, down_weight):
    normed = normalize(tokens, modality, norm_gain)
    block_normed = normed.reshape(N_EXPERT, TOK_DEV, D)
    block_ids = expert_ids.reshape(N_EXPERT, TOK_DEV, TOP)
    slots, owners = jax.vmap(lambda ids: slot_table(ids, EXPERTS, CAP))(block_ids)
    packed = jax.vmap(pack_rows)(block_normed, owners)
    per_expert = packed.reshape(N_EXPERT, EXPERTS, CAP, D).transpose(1, 0, 2, 3).reshape(EXPERTS, N_EXPERT * CAP, D)

    def run_one(index):
        start = (index * HIDDEN_SIZE).astype(jnp.int32)
        gate_cols = lax.dynamic_slice_in_dim(gate_weight, start, HIDDEN_SIZE, 1)
        up_cols = lax.dynamic_slice_in_dim(up_weight, start, HIDDEN_SIZE, 1)
        down_rows = lax.dynamic_slice_in_dim(down_weight, start, HIDDEN_SIZE, 0)
        rows = lax.dynamic_index_in_dim(per_expert, index, 0, keepdims=False)
        return expert_rows(rows, gate_cols, up_cols, down_rows).astype(jnp.bfloat16)
    outputs = lax.map(run_one, jnp.arange(EXPERTS, dtype=jnp.int32))
    by_block = outputs.reshape(EXPERTS, N_EXPERT, CAP, D).transpose(1, 0, 2, 3).reshape(N_EXPERT, EXPERTS * CAP, D)
    picked = jax.vmap(lambda table, where_to: jnp.take(table, where_to, axis=0))(by_block, slots)
    picked = picked.reshape(TOKENS, TOP, D).astype(jnp.float32)
    mixed = tokens.astype(jnp.float32) + lax.optimization_barrier(jnp.sum(route_weights[:, :, None] * picked, axis=1))
    return mixed.astype(jnp.bfloat16)
```

```python
import functools

import jax
import jax.numpy as jnp
from jax import lax
from jax.experimental import pallas as pl
from jax.experimental.pallas import tpu as pltpu
from jax.sharding import PartitionSpec as P

epsilon = 1e-05
LANES = 128
AXIS = "expert"


def grid_side(devices):
    side = 1
    while side * side < devices:
        side += 1
    return side if side * side == devices else devices


def moe_kernel(
    devices,
    tokens_hbm,
    modality_ref,
    ids_ref,
    weights_ref,
    gain_ref,
    gate_hbm,
    up_hbm,
    down_hbm,
    out_ref,
    tokens,
    gate,
    up,
    down,
    normed,
    total,
    place_rows,
    place_cols,
    share_cols,
    packed,
    arrived,
    finished,
    returned,
    load_sem,
    go_send,
    go_recv,
    back_send,
    back_recv,
):
    waves, _, chunk, width = packed.shape
    tok_rows = tokens.shape[0]
    fanout = ids_ref.shape[0]
    me = lax.axis_index(AXIS)
    side = grid_side(devices)
    mine_hi, mine_lo = me // side, me % side
    lines = devices // side

    def ahead(step):
        return ((mine_hi + step // side) % lines) * side + (mine_lo + step % side) % side

    def behind(step):
        return ((mine_hi + lines - step // side) % lines) * side + (
            mine_lo + side - step % side
        ) % side

    def go(wave, step):
        return pltpu.make_async_remote_copy(
            src_ref=packed.at[wave, step],
            dst_ref=arrived.at[wave, step],
            send_sem=go_send.at[wave, step],
            recv_sem=go_recv.at[wave, step],
            device_id={AXIS: ahead(step)},
            device_id_type=pl.DeviceIdType.MESH,
        )

    def back(wave, step):
        return pltpu.make_async_remote_copy(
            src_ref=finished.at[wave, step],
            dst_ref=returned.at[wave, step],
            send_sem=back_send.at[wave, step],
            recv_sem=back_recv.at[wave, step],
            device_id={AXIS: behind(step)},
            device_id_type=pl.DeviceIdType.MESH,
        )

    loads = [
        pltpu.make_async_copy(tokens_hbm, tokens, load_sem.at[0]),
        pltpu.make_async_copy(gate_hbm, gate, load_sem.at[1]),
        pltpu.make_async_copy(up_hbm, up, load_sem.at[2]),
        pltpu.make_async_copy(down_hbm, down, load_sem.at[3]),
    ]
    for load in loads:
        load.start()

    barrier = pltpu.get_barrier_semaphore()

    def greet(step, carry):
        pl.semaphore_signal(
            barrier, inc=1, device_id={AXIS: ahead(step)}, device_id_type=pl.DeviceIdType.MESH
        )
        return carry

    lax.fori_loop(1, devices, greet, 0)

    expert = lax.broadcasted_iota(jnp.int32, (LANES, tok_rows), 0)
    named = jnp.zeros((LANES, tok_rows), jnp.float32)
    share = jnp.zeros((LANES, tok_rows), jnp.float32)
    for k in range(fanout):
        hit = expert == ids_ref[k : k + 1, :]
        named = jnp.where(hit, 1.0, named)
        share = jnp.where(hit, weights_ref[k : k + 1, :], share)
    before = (
        lax.broadcasted_iota(jnp.int32, (tok_rows, tok_rows), 0)
        < lax.broadcasted_iota(jnp.int32, (tok_rows, tok_rows), 1)
    )
    count = jnp.dot(
        named.astype(jnp.bfloat16),
        jnp.where(before, 1.0, 0.0).astype(jnp.bfloat16),
        preferred_element_type=jnp.float32,
    )
    place = jnp.where(named > 0.5, count, -1.0)
    place_rows[...] = place
    place_cols[...] = place.T
    share_cols[...] = share.T
    image = jnp.broadcast_to(modality_ref[...].astype(jnp.float32), (LANES, tok_rows)).T

    loads[0].wait()
    rows = 64
    for start in range(0, tok_rows, rows):
        values = tokens[start : start + rows, :].astype(jnp.float32)
        square = jnp.mean(values * values, axis=1, keepdims=True)
        gains = jnp.where(
            image[start : start + rows, :1] > 0.5, gain_ref[1:2, :], gain_ref[0:1, :]
        )
        normed[start : start + rows, :] = (
            values * lax.rsqrt(square + epsilon) * gains
        ).astype(jnp.bfloat16)

    def pack(wave, step, target):
        line = place_rows[pl.ds(ahead(step), 1), :]
        slot = lax.broadcasted_iota(jnp.int32, (chunk, tok_rows), 0) + wave * chunk
        pick = jnp.where(line == slot.astype(jnp.float32), 1.0, 0.0).astype(jnp.bfloat16)
        target[wave, step] = jnp.dot(
            pick, normed[...], preferred_element_type=jnp.float32
        ).astype(jnp.bfloat16)

    others = devices - 1
    items = waves * others

    def which(item):
        return item // others, others - item % others

    pl.semaphore_wait(barrier, others)

    def send(item, carry):
        wave, step = which(item)
        pack(wave, step, packed)
        go(wave, step).start()
        return carry

    lax.fori_loop(0, items, send, 0)

    for load in loads[1:]:
        load.wait()

    def feed(source, target, wave, step):
        value = source[wave, step]
        opened = jnp.dot(value, gate[...], preferred_element_type=jnp.float32)
        upper = jnp.dot(value, up[...], preferred_element_type=jnp.float32)
        active = (opened / (1.0 + jnp.exp(-opened)) * upper).astype(jnp.bfloat16)
        target[wave, step] = jnp.dot(
            active, down[...], preferred_element_type=jnp.float32
        ).astype(jnp.bfloat16)

    def spread(wave, step):
        lane = lax.broadcasted_iota(jnp.int32, (tok_rows, LANES), 1) == ahead(step)
        line = jnp.sum(jnp.where(lane, place_cols[...], 0.0), axis=1, keepdims=True)
        worth = jnp.sum(jnp.where(lane, share_cols[...], 0.0), axis=1, keepdims=True)
        slot = lax.broadcasted_iota(jnp.int32, (tok_rows, chunk), 1) + wave * chunk
        spots = jnp.where(line == slot.astype(jnp.float32), worth, 0.0)
        high = spots.astype(jnp.bfloat16)
        low = (spots - high.astype(jnp.float32)).astype(jnp.bfloat16)
        value = returned[wave, step]
        return jnp.dot(high, value, preferred_element_type=jnp.float32) + jnp.dot(
            low, value, preferred_element_type=jnp.float32
        )

    total[...] = tokens[...].astype(jnp.float32)

    def local(wave, carry):
        pack(wave, 0, arrived)
        feed(arrived, returned, wave, 0)
        total[...] += spread(wave, 0)
        return carry

    lax.fori_loop(0, waves, local, 0)

    def serve(item, carry):
        wave, step = which(item)
        go(wave, step).wait_recv()
        feed(arrived, finished, wave, step)
        back(wave, step).start()
        return carry

    lax.fori_loop(0, items, serve, 0)

    def collect(item, carry):
        wave, step = which(item)
        back(wave, step).wait_recv()
        total[...] += spread(wave, step)
        return carry

    lax.fori_loop(0, items - 1, collect, 0)
    wave, step = which(items - 1)
    back(wave, step).wait_recv()
    out_ref[...] = (total[...] + spread(wave, step)).astype(out_ref.dtype)

    def settle(item, carry):
        wave, step = which(item)
        go(wave, step).wait_send()
        back(wave, step).wait_send()
        return carry

    lax.fori_loop(0, items, settle, 0)


def shards(
    tokens, modality, expert_ids, route_weights, norm_gain, gate_weight, up_weight, down_weight
):
    devices = lax.axis_size(AXIS)
    tok_rows, width = tokens.shape
    fanout = expert_ids.shape[1]
    hidden = gate_weight.shape[1]
    capacity = min(tok_rows, tok_rows * fanout * 5 // (4 * devices))
    waves = 2 if capacity % 32 == 0 and capacity >= 256 else 1
    chunk = capacity // waves
    buffer = pltpu.VMEM((waves, devices, chunk, width), jnp.bfloat16)
    near = pl.BlockSpec(memory_space=pltpu.VMEM)
    far = pl.BlockSpec(memory_space=pl.ANY)
    sems = pltpu.SemaphoreType.DMA((waves, devices))
    return pl.pallas_call(
        functools.partial(moe_kernel, devices),
        out_shape=jax.ShapeDtypeStruct((tok_rows, width), jnp.bfloat16),
        in_specs=[far, near, near, near, near, far, far, far],
        out_specs=near,
        scratch_shapes=[
            pltpu.VMEM((tok_rows, width), jnp.bfloat16),
            pltpu.VMEM((width, hidden), jnp.bfloat16),
            pltpu.VMEM((width, hidden), jnp.bfloat16),
            pltpu.VMEM((hidden, width), jnp.bfloat16),
            pltpu.VMEM((tok_rows, width), jnp.bfloat16),
            pltpu.VMEM((tok_rows, width), jnp.float32),
            pltpu.VMEM((LANES, tok_rows), jnp.float32),
            pltpu.VMEM((tok_rows, LANES), jnp.float32),
            pltpu.VMEM((tok_rows, LANES), jnp.float32),
            buffer,
            buffer,
            buffer,
            buffer,
            pltpu.SemaphoreType.DMA((4,)),
            sems,
            sems,
            sems,
            sems,
        ],
        compiler_params=pltpu.CompilerParams(
            collective_id=0, has_side_effects=True, vmem_limit_bytes=62 * 1024 * 1024
        ),
    )(
        tokens,
        modality.reshape(1, tok_rows),
        expert_ids.T,
        route_weights.T,
        norm_gain,
        gate_weight,
        up_weight,
        down_weight,
    )


def solution(mesh):
    placed = (
        P(("dp", AXIS), None),
        P(("dp", AXIS)),
        P(("dp", AXIS), None),
        P(("dp", AXIS), None),
        P(),
        P(None, AXIS),
        P(None, AXIS),
        P(AXIS, None),
    )
    return jax.shard_map(
        shards, mesh=mesh, in_specs=placed, out_specs=P(("dp", AXIS), None), check_vma=False
    )
```

```python
import functools

import jax
import jax.numpy as jnp
from jax import lax
from jax.experimental import pallas as pl
from jax.experimental.pallas import tpu as pltpu
from jax.sharding import PartitionSpec as P

epsilon = 1e-05
LANES = 128
AXIS = "expert"


def grid_side(devices):
    side = 1
    while side * side < devices:
        side += 1
    return side if side * side == devices else devices


def moe_kernel(
    devices,
    tokens_hbm,
    modality_ref,
    ids_ref,
    weights_ref,
    gain_ref,
    gate_hbm,
    up_hbm,
    down_hbm,
    out_ref,
    tokens,
    gate,
    up,
    down,
    normed,
    total,
    place_rows,
    place_cols,
    share_cols,
    packed,
    arrived,
    finished,
    returned,
    load_sem,
    go_send,
    go_recv,
    back_send,
    back_recv,
):
    waves, _, chunk, width = packed.shape
    tok_rows = tokens.shape[0]
    fanout = ids_ref.shape[0]
    me = lax.axis_index(AXIS)
    side = grid_side(devices)
    mine_hi, mine_lo = me // side, me % side
    lines = devices // side

    def ahead(step):
        return ((mine_hi + step // side) % lines) * side + (mine_lo + step % side) % side

    def behind(step):
        return ((mine_hi + lines - step // side) % lines) * side + (
            mine_lo + side - step % side
        ) % side

    def go(wave, step):
        return pltpu.make_async_remote_copy(
            src_ref=packed.at[wave, step],
            dst_ref=arrived.at[wave, step],
            send_sem=go_send.at[wave, step],
            recv_sem=go_recv.at[wave, step],
            device_id={AXIS: ahead(step)},
            device_id_type=pl.DeviceIdType.MESH,
        )

    def back(wave, step):
        return pltpu.make_async_remote_copy(
            src_ref=finished.at[wave, step],
            dst_ref=returned.at[wave, step],
            send_sem=back_send.at[wave, step],
            recv_sem=back_recv.at[wave, step],
            device_id={AXIS: behind(step)},
            device_id_type=pl.DeviceIdType.MESH,
        )

    loads = [
        pltpu.make_async_copy(tokens_hbm, tokens, load_sem.at[0]),
        pltpu.make_async_copy(gate_hbm, gate, load_sem.at[1]),
        pltpu.make_async_copy(up_hbm, up, load_sem.at[2]),
        pltpu.make_async_copy(down_hbm, down, load_sem.at[3]),
    ]
    for load in loads:
        load.start()

    barrier = pltpu.get_barrier_semaphore()

    def greet(step, carry):
        pl.semaphore_signal(
            barrier, inc=1, device_id={AXIS: ahead(step)}, device_id_type=pl.DeviceIdType.MESH
        )
        return carry

    lax.fori_loop(1, devices, greet, 0)

    expert = lax.broadcasted_iota(jnp.int32, (LANES, tok_rows), 0)
    named = jnp.zeros((LANES, tok_rows), jnp.float32)
    share = jnp.zeros((LANES, tok_rows), jnp.float32)
    for k in range(fanout):
        hit = expert == ids_ref[k : k + 1, :]
        named = jnp.where(hit, 1.0, named)
        share = jnp.where(hit, weights_ref[k : k + 1, :], share)
    before = (
        lax.broadcasted_iota(jnp.int32, (tok_rows, tok_rows), 0)
        < lax.broadcasted_iota(jnp.int32, (tok_rows, tok_rows), 1)
    )
    count = jnp.dot(
        named.astype(jnp.bfloat16),
        jnp.where(before, 1.0, 0.0).astype(jnp.bfloat16),
        preferred_element_type=jnp.float32,
    )
    place = jnp.where(named > 0.5, count, -1.0)
    place_rows[...] = place
    place_cols[...] = place.T
    share_cols[...] = share.T
    image = jnp.broadcast_to(modality_ref[...].astype(jnp.float32), (LANES, tok_rows)).T

    loads[0].wait()
    rows = 64
    for start in range(0, tok_rows, rows):
        values = tokens[start : start + rows, :].astype(jnp.float32)
        square = jnp.mean(values * values, axis=1, keepdims=True)
        gains = jnp.where(
            image[start : start + rows, :1] > 0.5, gain_ref[1:2, :], gain_ref[0:1, :]
        )
        normed[start : start + rows, :] = (
            values * lax.rsqrt(square + epsilon) * gains
        ).astype(jnp.bfloat16)

    def pack(wave, step, target):
        line = place_rows[pl.ds(ahead(step), 1), :]
        slot = lax.broadcasted_iota(jnp.int32, (chunk, tok_rows), 0) + wave * chunk
        pick = jnp.where(line == slot.astype(jnp.float32), 1.0, 0.0).astype(jnp.bfloat16)
        target[wave, step] = jnp.dot(
            pick, normed[...], preferred_element_type=jnp.float32
        ).astype(jnp.bfloat16)

    others = devices - 1
    items = waves * others

    def which(item):
        return item // others, others - item % others

    pl.semaphore_wait(barrier, others)

    def send(item, carry):
        wave, step = which(item)
        pack(wave, step, packed)
        go(wave, step).start()
        return carry

    lax.fori_loop(0, items, send, 0)

    for load in loads[1:]:
        load.wait()

    def feed(source, target, wave, step):
        value = source[wave, step]
        opened = jnp.dot(value, gate[...], preferred_element_type=jnp.float32)
        upper = jnp.dot(value, up[...], preferred_element_type=jnp.float32)
        active = (opened / (1.0 + jnp.exp(-opened)) * upper).astype(jnp.bfloat16)
        target[wave, step] = jnp.dot(
            active, down[...], preferred_element_type=jnp.float32
        ).astype(jnp.bfloat16)

    def spread(wave, step):
        lane = lax.broadcasted_iota(jnp.int32, (tok_rows, LANES), 1) == ahead(step)
        line = jnp.sum(jnp.where(lane, place_cols[...], 0.0), axis=1, keepdims=True)
        worth = jnp.sum(jnp.where(lane, share_cols[...], 0.0), axis=1, keepdims=True)
        slot = lax.broadcasted_iota(jnp.int32, (tok_rows, chunk), 1) + wave * chunk
        spots = jnp.where(line == slot.astype(jnp.float32), worth, 0.0)
        high = spots.astype(jnp.bfloat16)
        low = (spots - high.astype(jnp.float32)).astype(jnp.bfloat16)
        value = returned[wave, step]
        return jnp.dot(high, value, preferred_element_type=jnp.float32) + jnp.dot(
            low, value, preferred_element_type=jnp.float32
        )

    total[...] = tokens[...].astype(jnp.float32)

    def local(wave, carry):
        pack(wave, 0, arrived)
        feed(arrived, returned, wave, 0)
        total[...] += spread(wave, 0)
        return carry

    lax.fori_loop(0, waves, local, 0)

    def serve(item, carry):
        wave, step = which(item)
        go(wave, step).wait_recv()
        feed(arrived, finished, wave, step)
        back(wave, step).start()
        return carry

    lax.fori_loop(0, items, serve, 0)

    def collect(item, carry):
        wave, step = which(item)
        back(wave, step).wait_recv()
        total[...] += spread(wave, step)
        return carry

    lax.fori_loop(0, items - 1, collect, 0)
    wave, step = which(items - 1)
    back(wave, step).wait_recv()
    out_ref[...] = (total[...] + spread(wave, step)).astype(out_ref.dtype)

    def settle(item, carry):
        wave, step = which(item)
        go(wave, step).wait_send()
        back(wave, step).wait_send()
        return carry

    lax.fori_loop(0, items, settle, 0)


def relay_kernel(
    blocks,
    tokens_hbm,
    modality_ref,
    ids_ref,
    weights_ref,
    gain_ref,
    gate_hbm,
    up_hbm,
    down_hbm,
    out_ref,
    tokens,
    near_tokens,
    gate,
    up,
    down,
    normed,
    near_normed,
    total,
    near_total,
    facts,
    near_facts,
    packed,
    arrived,
    finished,
    returned,
    own_rows,
    own_results,
    sum_out,
    sum_in,
    load_sem,
    facts_sem,
    dense_send,
    dense_recv,
    go_send,
    go_recv,
    back_send,
    back_recv,
    sum_send,
    sum_recv,
):
    _, capacity, width = packed.shape
    waves = go_send.shape[1]
    chunk = capacity // waves
    tok_rows = tokens.shape[0]
    part = tok_rows // blocks
    fanout = ids_ref.shape[0]
    me = lax.axis_index(AXIS)
    role = lax.axis_index("dp") % 2
    high, low = me // 2, me % 2
    beside = high * 2 + 1 - low
    above = (1 - high) * 2 + low
    first = beside * (1 - role) + above * role
    second = above * (1 - role) + beside * role

    def remote(source, target, send_sem, recv_sem, peer):
        return pltpu.make_async_remote_copy(
            src_ref=source,
            dst_ref=target,
            send_sem=send_sem,
            recv_sem=recv_sem,
            device_id={AXIS: peer},
            device_id_type=pl.DeviceIdType.MESH,
        )

    def part_rows(block):
        return pl.ds(pl.multiple_of(block * part, part), part)

    def wave_rows(wave):
        return pl.ds(pl.multiple_of(wave * chunk, chunk), chunk)

    def dense(block):
        rows = part_rows(block)
        return remote(
            tokens.at[rows], near_tokens.at[rows], dense_send.at[block], dense_recv.at[block], first
        )

    def go(kind, wave):
        rows = wave_rows(wave)
        return remote(
            packed.at[kind, rows],
            arrived.at[kind, rows],
            go_send.at[kind, wave],
            go_recv.at[kind, wave],
            second,
        )

    def back(kind, wave):
        rows = wave_rows(wave)
        return remote(
            finished.at[kind, rows],
            returned.at[kind, rows],
            back_send.at[kind, wave],
            back_recv.at[kind, wave],
            second,
        )

    def sums(block):
        rows = part_rows(block)
        return remote(
            sum_out.at[rows], sum_in.at[rows], sum_send.at[block], sum_recv.at[block], first
        )

    def each(count, step):
        def body(index, carry):
            step(index)
            return carry

        lax.fori_loop(0, count, body, 0)

    loads = [
        pltpu.make_async_copy(tokens_hbm, tokens, load_sem.at[0]),
        pltpu.make_async_copy(gate_hbm, gate, load_sem.at[1]),
        pltpu.make_async_copy(up_hbm, up, load_sem.at[2]),
        pltpu.make_async_copy(down_hbm, down, load_sem.at[3]),
    ]
    loads[0].start()
    barrier = pltpu.get_barrier_semaphore()
    for peer in (first, second):
        pl.semaphore_signal(
            barrier, inc=1, device_id={AXIS: peer}, device_id_type=pl.DeviceIdType.MESH
        )
    loads[0].wait()
    pl.semaphore_wait(barrier, 2)
    each(blocks, lambda block: dense(block).start())
    for load in loads[1:]:
        load.start()

    lines = 8
    expert = lax.broadcasted_iota(jnp.int32, (lines, tok_rows), 0)
    named = jnp.zeros((lines, tok_rows), jnp.float32)
    share = jnp.zeros((lines, tok_rows), jnp.float32)
    for k in range(fanout):
        hit = expert == ids_ref[k : k + 1, :]
        named = jnp.where(hit, 1.0, named)
        share = jnp.where(hit, weights_ref[k : k + 1, :], share)
    before = (
        lax.broadcasted_iota(jnp.int32, (tok_rows, tok_rows), 0)
        < lax.broadcasted_iota(jnp.int32, (tok_rows, tok_rows), 1)
    )
    count = jnp.dot(
        named.astype(jnp.bfloat16),
        jnp.where(before, 1.0, 0.0).astype(jnp.bfloat16),
        preferred_element_type=jnp.float32,
    )
    facts[0:lines, :] = jnp.where(named > 0.5, count, -1.0)
    facts[lines : 2 * lines, :] = share
    facts[2 * lines : 3 * lines, :] = jnp.broadcast_to(
        modality_ref[...].astype(jnp.float32), (lines, tok_rows)
    )
    told = remote(facts, near_facts, facts_sem.at[0], facts_sem.at[1], first)
    told.start()

    def column(line):
        return jnp.broadcast_to(line, (LANES, tok_rows)).T[:, :1]

    def normalize_rows(source, target, image, start, rows):
        values = source[start : start + rows, :].astype(jnp.float32)
        square = jnp.mean(values * values, axis=1, keepdims=True)
        gains = jnp.where(
            image[start : start + rows] > 0.5, gain_ref[1:2, :], gain_ref[0:1, :]
        )
        target[start : start + rows, :] = (
            values * lax.rsqrt(square + epsilon) * gains
        ).astype(jnp.bfloat16)

    def pack(notes, rows, who, wave):
        line = notes[pl.ds(who, 1), :]
        slot = lax.broadcasted_iota(jnp.int32, (chunk, tok_rows), 0) + wave * chunk
        pick = jnp.where(line == slot.astype(jnp.float32), 1.0, 0.0).astype(jnp.bfloat16)
        return jnp.dot(pick, rows[...], preferred_element_type=jnp.float32).astype(jnp.bfloat16)

    def feed(value):
        opened = jnp.dot(value, gate[...], preferred_element_type=jnp.float32)
        upper = jnp.dot(value, up[...], preferred_element_type=jnp.float32)
        active = (opened / (1.0 + jnp.exp(-opened)) * upper).astype(jnp.bfloat16)
        return jnp.dot(active, down[...], preferred_element_type=jnp.float32).astype(jnp.bfloat16)

    def spots(notes, who):
        line = column(notes[pl.ds(who, 1), :])
        worth = column(notes[pl.ds(who + lines, 1), :])
        slot = lax.broadcasted_iota(jnp.int32, (tok_rows, capacity), 1)
        full = jnp.where(line == slot.astype(jnp.float32), worth, 0.0)
        coarse = full.astype(jnp.bfloat16)
        return coarse, (full - coarse.astype(jnp.float32)).astype(jnp.bfloat16)

    def spread(coarse, fine, value):
        return jnp.dot(coarse, value, preferred_element_type=jnp.float32) + jnp.dot(
            fine, value, preferred_element_type=jnp.float32
        )

    image = column(facts[2 * lines : 2 * lines + 1, :])
    rows = 64
    for start in range(0, tok_rows, rows):
        normalize_rows(tokens, normed, image, start, rows)

    def send(wave):
        packed[0, wave_rows(wave)] = pack(facts, normed, second, wave)
        go(0, wave).start()

    each(waves, send)

    for load in loads[1:]:
        load.wait()

    def local(wave):
        here = wave_rows(wave)
        own_results[here] = feed(pack(facts, normed, me, wave))

    each(waves, local)
    total[...] = tokens[...].astype(jnp.float32) + spread(*spots(facts, me), own_results[...])

    def serve(kind):
        def step(wave):
            here = wave_rows(wave)
            go(kind, wave).wait_recv()
            finished[kind, here] = feed(arrived[kind, here])
            back(kind, wave).start()

        each(waves, step)

    serve(0)

    told.wait_recv()
    near_image = column(near_facts[2 * lines : 2 * lines + 1, :])
    for block in range(blocks):
        dense(block).wait_recv()
        for start in range(block * part, (block + 1) * part, rows):
            normalize_rows(near_tokens, near_normed, near_image, start, rows)

    def forward(wave):
        packed[1, wave_rows(wave)] = pack(near_facts, near_normed, second, wave)
        go(1, wave).start()

    each(waves, forward)

    def near_local(wave):
        here = wave_rows(wave)
        own_rows[here] = feed(pack(near_facts, near_normed, me, wave))

    each(waves, near_local)
    near_total[...] = spread(*spots(near_facts, me), own_rows[...])

    serve(1)

    each(waves, lambda wave: back(0, wave).wait_recv())
    total[...] += spread(*spots(facts, second), returned[0])

    coarse, fine = spots(near_facts, second)
    each(waves, lambda wave: back(1, wave).wait_recv())
    for block in range(blocks):
        here = slice(block * part, (block + 1) * part)
        sum_out[here, :] = (
            near_total[here, :] + spread(coarse[here], fine[here], returned[1])
        ).astype(jnp.bfloat16)
        sums(block).start()

    for block in range(blocks):
        here = slice(block * part, (block + 1) * part)
        sums(block).wait_recv()
        out_ref[here, :] = (total[here, :] + sum_in[here, :].astype(jnp.float32)).astype(
            out_ref.dtype
        )

    told.wait_send()
    each(blocks, lambda block: dense(block).wait_send())
    each(blocks, lambda block: sums(block).wait_send())
    for kind in range(2):
        each(waves, lambda wave: go(kind, wave).wait_send())
        each(waves, lambda wave: back(kind, wave).wait_send())


def relay_scratch(tok_rows, width, hidden, capacity, waves, blocks):
    dense = pltpu.VMEM((tok_rows, width), jnp.bfloat16)
    sums = pltpu.VMEM((tok_rows, width), jnp.float32)
    facts = pltpu.VMEM((24, tok_rows), jnp.float32)
    slots = pltpu.VMEM((2, capacity, width), jnp.bfloat16)
    single = pltpu.VMEM((capacity, width), jnp.bfloat16)
    wide = pltpu.VMEM((width, hidden), jnp.bfloat16)
    by_block = pltpu.SemaphoreType.DMA((blocks,))
    by_wave = pltpu.SemaphoreType.DMA((2, waves))
    return [
        dense, dense, wide, wide, pltpu.VMEM((hidden, width), jnp.bfloat16), dense, dense,
        sums, sums, facts, facts, slots, slots, slots, slots, single, single, dense, dense,
        pltpu.SemaphoreType.DMA((4,)), pltpu.SemaphoreType.DMA((2,)), by_block, by_block,
        by_wave, by_wave, by_wave, by_wave, by_block, by_block,
    ]


def direct_scratch(tok_rows, width, hidden, buffer, sems):
    return [
        pltpu.VMEM((tok_rows, width), jnp.bfloat16),
        pltpu.VMEM((width, hidden), jnp.bfloat16),
        pltpu.VMEM((width, hidden), jnp.bfloat16),
        pltpu.VMEM((hidden, width), jnp.bfloat16),
        pltpu.VMEM((tok_rows, width), jnp.bfloat16),
        pltpu.VMEM((tok_rows, width), jnp.float32),
        pltpu.VMEM((LANES, tok_rows), jnp.float32),
        pltpu.VMEM((tok_rows, LANES), jnp.float32),
        pltpu.VMEM((tok_rows, LANES), jnp.float32),
        buffer,
        buffer,
        buffer,
        buffer,
        pltpu.SemaphoreType.DMA((4,)),
        sems,
        sems,
        sems,
        sems,
    ]


def shards(
    tokens, modality, expert_ids, route_weights, norm_gain, gate_weight, up_weight, down_weight
):
    devices = lax.axis_size(AXIS)
    tok_rows, width = tokens.shape
    fanout = expert_ids.shape[1]
    hidden = gate_weight.shape[1]
    capacity = min(tok_rows, tok_rows * fanout * 5 // (4 * devices))
    waves = 2 if capacity % 32 == 0 and capacity >= 256 else 1
    chunk = capacity // waves
    buffer = pltpu.VMEM((waves, devices, chunk, width), jnp.bfloat16)
    near = pl.BlockSpec(memory_space=pltpu.VMEM)
    far = pl.BlockSpec(memory_space=pl.ANY)
    sems = pltpu.SemaphoreType.DMA((waves, devices))
    blocks = 4
    relayed = devices == 4 and tok_rows % (64 * blocks) == 0 and capacity % 32 == 0
    if relayed:
        kernel = functools.partial(relay_kernel, blocks)
        scratch = relay_scratch(tok_rows, width, hidden, capacity, 2, blocks)
    else:
        kernel = functools.partial(moe_kernel, devices)
        scratch = direct_scratch(tok_rows, width, hidden, buffer, sems)
    return pl.pallas_call(
        kernel,
        out_shape=jax.ShapeDtypeStruct((tok_rows, width), jnp.bfloat16),
        in_specs=[far, near, near, near, near, far, far, far],
        out_specs=near,
        scratch_shapes=scratch,
        compiler_params=pltpu.CompilerParams(
            collective_id=0, has_side_effects=True, vmem_limit_bytes=62 * 1024 * 1024
        ),
    )(
        tokens,
        modality.reshape(1, tok_rows),
        expert_ids.T,
        route_weights.T,
        norm_gain,
        gate_weight,
        up_weight,
        down_weight,
    )


def solution(mesh):
    placed = (
        P(("dp", AXIS), None),
        P(("dp", AXIS)),
        P(("dp", AXIS), None),
        P(("dp", AXIS), None),
        P(),
        P(None, AXIS),
        P(None, AXIS),
        P(AXIS, None),
    )
    return jax.shard_map(
        shards, mesh=mesh, in_specs=placed, out_specs=P(("dp", AXIS), None), check_vma=False
    )
```

```python
import functools

import jax
import jax.numpy as jnp
from jax import lax
from jax.experimental import pallas as pl
from jax.experimental.pallas import tpu as pltpu
from jax.sharding import PartitionSpec as P

epsilon = 1e-05
LANES = 128
AXIS = "expert"


def grid_side(devices):
    side = 1
    while side * side < devices:
        side += 1
    return side if side * side == devices else devices


def moe_kernel(
    devices,
    tokens_hbm,
    modality_ref,
    ids_ref,
    weights_ref,
    gain_ref,
    gate_hbm,
    up_hbm,
    down_hbm,
    out_ref,
    tokens,
    gate,
    up,
    down,
    normed,
    total,
    place_rows,
    place_cols,
    share_cols,
    packed,
    arrived,
    finished,
    returned,
    load_sem,
    go_send,
    go_recv,
    back_send,
    back_recv,
):
    waves, _, chunk, width = packed.shape
    tok_rows = tokens.shape[0]
    fanout = ids_ref.shape[0]
    me = lax.axis_index(AXIS)
    side = grid_side(devices)
    mine_hi, mine_lo = me // side, me % side
    lines = devices // side

    def ahead(step):
        return ((mine_hi + step // side) % lines) * side + (mine_lo + step % side) % side

    def behind(step):
        return ((mine_hi + lines - step // side) % lines) * side + (
            mine_lo + side - step % side
        ) % side

    def go(wave, step):
        return pltpu.make_async_remote_copy(
            src_ref=packed.at[wave, step],
            dst_ref=arrived.at[wave, step],
            send_sem=go_send.at[wave, step],
            recv_sem=go_recv.at[wave, step],
            device_id={AXIS: ahead(step)},
            device_id_type=pl.DeviceIdType.MESH,
        )

    def back(wave, step):
        return pltpu.make_async_remote_copy(
            src_ref=finished.at[wave, step],
            dst_ref=returned.at[wave, step],
            send_sem=back_send.at[wave, step],
            recv_sem=back_recv.at[wave, step],
            device_id={AXIS: behind(step)},
            device_id_type=pl.DeviceIdType.MESH,
        )

    loads = [
        pltpu.make_async_copy(tokens_hbm, tokens, load_sem.at[0]),
        pltpu.make_async_copy(gate_hbm, gate, load_sem.at[1]),
        pltpu.make_async_copy(up_hbm, up, load_sem.at[2]),
        pltpu.make_async_copy(down_hbm, down, load_sem.at[3]),
    ]
    for load in loads:
        load.start()

    barrier = pltpu.get_barrier_semaphore()

    def greet(step, carry):
        pl.semaphore_signal(
            barrier, inc=1, device_id={AXIS: ahead(step)}, device_id_type=pl.DeviceIdType.MESH
        )
        return carry

    lax.fori_loop(1, devices, greet, 0)

    expert = lax.broadcasted_iota(jnp.int32, (LANES, tok_rows), 0)
    named = jnp.zeros((LANES, tok_rows), jnp.float32)
    share = jnp.zeros((LANES, tok_rows), jnp.float32)
    for k in range(fanout):
        hit = expert == ids_ref[k : k + 1, :]
        named = jnp.where(hit, 1.0, named)
        share = jnp.where(hit, weights_ref[k : k + 1, :], share)
    before = (
        lax.broadcasted_iota(jnp.int32, (tok_rows, tok_rows), 0)
        < lax.broadcasted_iota(jnp.int32, (tok_rows, tok_rows), 1)
    )
    count = jnp.dot(
        named.astype(jnp.bfloat16),
        jnp.where(before, 1.0, 0.0).astype(jnp.bfloat16),
        preferred_element_type=jnp.float32,
    )
    place = jnp.where(named > 0.5, count, -1.0)
    place_rows[...] = place
    place_cols[...] = place.T
    share_cols[...] = share.T
    image = jnp.broadcast_to(modality_ref[...].astype(jnp.float32), (LANES, tok_rows)).T

    loads[0].wait()
    rows = 64
    for start in range(0, tok_rows, rows):
        values = tokens[start : start + rows, :].astype(jnp.float32)
        square = jnp.mean(values * values, axis=1, keepdims=True)
        gains = jnp.where(
            image[start : start + rows, :1] > 0.5, gain_ref[1:2, :], gain_ref[0:1, :]
        )
        normed[start : start + rows, :] = (
            values * lax.rsqrt(square + epsilon) * gains
        ).astype(jnp.bfloat16)

    def pack(wave, step, target):
        line = place_rows[pl.ds(ahead(step), 1), :]
        slot = lax.broadcasted_iota(jnp.int32, (chunk, tok_rows), 0) + wave * chunk
        pick = jnp.where(line == slot.astype(jnp.float32), 1.0, 0.0).astype(jnp.bfloat16)
        target[wave, step] = jnp.dot(
            pick, normed[...], preferred_element_type=jnp.float32
        ).astype(jnp.bfloat16)

    others = devices - 1
    items = waves * others

    def which(item):
        return item // others, others - item % others

    pl.semaphore_wait(barrier, others)

    def send(item, carry):
        wave, step = which(item)
        pack(wave, step, packed)
        go(wave, step).start()
        return carry

    lax.fori_loop(0, items, send, 0)

    for load in loads[1:]:
        load.wait()

    def feed(source, target, wave, step):
        value = source[wave, step]
        opened = jnp.dot(value, gate[...], preferred_element_type=jnp.float32)
        upper = jnp.dot(value, up[...], preferred_element_type=jnp.float32)
        active = (opened / (1.0 + jnp.exp(-opened)) * upper).astype(jnp.bfloat16)
        target[wave, step] = jnp.dot(
            active, down[...], preferred_element_type=jnp.float32
        ).astype(jnp.bfloat16)

    def spread(wave, step):
        lane = lax.broadcasted_iota(jnp.int32, (tok_rows, LANES), 1) == ahead(step)
        line = jnp.sum(jnp.where(lane, place_cols[...], 0.0), axis=1, keepdims=True)
        worth = jnp.sum(jnp.where(lane, share_cols[...], 0.0), axis=1, keepdims=True)
        slot = lax.broadcasted_iota(jnp.int32, (tok_rows, chunk), 1) + wave * chunk
        spots = jnp.where(line == slot.astype(jnp.float32), worth, 0.0)
        high = spots.astype(jnp.bfloat16)
        low = (spots - high.astype(jnp.float32)).astype(jnp.bfloat16)
        value = returned[wave, step]
        return jnp.dot(high, value, preferred_element_type=jnp.float32) + jnp.dot(
            low, value, preferred_element_type=jnp.float32
        )

    total[...] = tokens[...].astype(jnp.float32)

    def local(wave, carry):
        pack(wave, 0, arrived)
        feed(arrived, returned, wave, 0)
        total[...] += spread(wave, 0)
        return carry

    lax.fori_loop(0, waves, local, 0)

    def serve(item, carry):
        wave, step = which(item)
        go(wave, step).wait_recv()
        feed(arrived, finished, wave, step)
        back(wave, step).start()
        return carry

    lax.fori_loop(0, items, serve, 0)

    def collect(item, carry):
        wave, step = which(item)
        back(wave, step).wait_recv()
        total[...] += spread(wave, step)
        return carry

    lax.fori_loop(0, items - 1, collect, 0)
    wave, step = which(items - 1)
    back(wave, step).wait_recv()
    out_ref[...] = (total[...] + spread(wave, step)).astype(out_ref.dtype)

    def settle(item, carry):
        wave, step = which(item)
        go(wave, step).wait_send()
        back(wave, step).wait_send()
        return carry

    lax.fori_loop(0, items, settle, 0)


def relay_kernel(
    blocks,
    tokens_hbm,
    modality_hbm,
    ids_hbm,
    weights_hbm,
    gain_hbm,
    gate_hbm,
    up_hbm,
    down_hbm,
    out_ref,
    modality_ref,
    ids_ref,
    weights_ref,
    gain_ref,
    tokens,
    near_tokens,
    gate,
    up,
    down,
    normed,
    near_normed,
    total,
    near_total,
    facts,
    near_facts,
    packed,
    arrived,
    finished,
    returned,
    own_rows,
    own_results,
    sum_out,
    sum_in,
    load_sem,
    token_sem,
    facts_sem,
    dense_send,
    dense_recv,
    go_send,
    go_recv,
    back_send,
    back_recv,
    sum_send,
    sum_recv,
):
    _, capacity, width = packed.shape
    waves = go_send.shape[1]
    chunk = capacity // waves
    tok_rows = tokens.shape[0]
    part = tok_rows // blocks
    fanout = ids_ref.shape[0]
    me = lax.axis_index(AXIS)
    role = lax.axis_index("dp") % 2
    high, low = me // 2, me % 2
    beside = high * 2 + 1 - low
    above = (1 - high) * 2 + low
    first = beside * (1 - role) + above * role
    second = above * (1 - role) + beside * role

    def remote(source, target, send_sem, recv_sem, peer):
        return pltpu.make_async_remote_copy(
            src_ref=source,
            dst_ref=target,
            send_sem=send_sem,
            recv_sem=recv_sem,
            device_id={AXIS: peer},
            device_id_type=pl.DeviceIdType.MESH,
        )

    def part_rows(block):
        return pl.ds(pl.multiple_of(block * part, part), part)

    def wave_rows(wave):
        return pl.ds(pl.multiple_of(wave * chunk, chunk), chunk)

    def dense(block):
        rows = part_rows(block)
        return remote(
            tokens.at[rows], near_tokens.at[rows], dense_send.at[block], dense_recv.at[block], first
        )

    def go(kind, wave):
        rows = wave_rows(wave)
        return remote(
            packed.at[kind, rows],
            arrived.at[kind, rows],
            go_send.at[kind, wave],
            go_recv.at[kind, wave],
            second,
        )

    def back(kind, wave):
        rows = wave_rows(wave)
        return remote(
            finished.at[kind, rows],
            returned.at[kind, rows],
            back_send.at[kind, wave],
            back_recv.at[kind, wave],
            second,
        )

    def sums(block):
        rows = part_rows(block)
        return remote(
            sum_out.at[rows], sum_in.at[rows], sum_send.at[block], sum_recv.at[block], first
        )

    def each(count, step):
        def body(index, carry):
            step(index)
            return carry

        lax.fori_loop(0, count, body, 0)

    loads = [
        pltpu.make_async_copy(source, target, load_sem.at[index])
        for index, (source, target) in enumerate(
            (
                (ids_hbm, ids_ref),
                (weights_hbm, weights_ref),
                (modality_hbm, modality_ref),
                (gain_hbm, gain_ref),
                (gate_hbm, gate),
                (up_hbm, up),
                (down_hbm, down),
            )
        )
    ]

    def token_load(block):
        rows = part_rows(block)
        return pltpu.make_async_copy(tokens_hbm.at[rows], tokens.at[rows], token_sem.at[block])

    each(blocks, lambda block: token_load(block).start())
    for load in loads[:4]:
        load.start()
    barrier = pltpu.get_barrier_semaphore()
    for peer in (first, second):
        pl.semaphore_signal(
            barrier, inc=1, device_id={AXIS: peer}, device_id_type=pl.DeviceIdType.MESH
        )
    pl.semaphore_wait(barrier, 2)

    def leave(block):
        token_load(block).wait()
        dense(block).start()

    each(blocks, leave)
    for load in loads[4:]:
        load.start()
    for load in loads[:4]:
        load.wait()

    lines = 8
    expert = lax.broadcasted_iota(jnp.int32, (lines, tok_rows), 0)
    named = jnp.zeros((lines, tok_rows), jnp.float32)
    share = jnp.zeros((lines, tok_rows), jnp.float32)
    for k in range(fanout):
        hit = expert == ids_ref[k : k + 1, :]
        named = jnp.where(hit, 1.0, named)
        share = jnp.where(hit, weights_ref[k : k + 1, :], share)
    before = (
        lax.broadcasted_iota(jnp.int32, (tok_rows, tok_rows), 0)
        < lax.broadcasted_iota(jnp.int32, (tok_rows, tok_rows), 1)
    )
    count = jnp.dot(
        named.astype(jnp.bfloat16),
        jnp.where(before, 1.0, 0.0).astype(jnp.bfloat16),
        preferred_element_type=jnp.float32,
    )
    facts[0:lines, :] = jnp.where(named > 0.5, count, -1.0)
    facts[lines : 2 * lines, :] = share
    facts[2 * lines : 3 * lines, :] = jnp.broadcast_to(
        modality_ref[...].astype(jnp.float32), (lines, tok_rows)
    )
    told = remote(facts, near_facts, facts_sem.at[0], facts_sem.at[1], first)
    told.start()

    def column(line):
        return jnp.broadcast_to(line, (LANES, tok_rows)).T[:, :1]

    def normalize_rows(source, target, image, start, rows):
        values = source[start : start + rows, :].astype(jnp.float32)
        square = jnp.mean(values * values, axis=1, keepdims=True)
        gains = jnp.where(
            image[start : start + rows] > 0.5, gain_ref[1:2, :], gain_ref[0:1, :]
        )
        target[start : start + rows, :] = (
            values * lax.rsqrt(square + epsilon) * gains
        ).astype(jnp.bfloat16)

    def pack(notes, rows, who, wave):
        line = notes[pl.ds(who, 1), :]
        slot = lax.broadcasted_iota(jnp.int32, (chunk, tok_rows), 0) + wave * chunk
        pick = jnp.where(line == slot.astype(jnp.float32), 1.0, 0.0).astype(jnp.bfloat16)
        return jnp.dot(pick, rows[...], preferred_element_type=jnp.float32).astype(jnp.bfloat16)

    def feed(value):
        opened = jnp.dot(value, gate[...], preferred_element_type=jnp.float32)
        upper = jnp.dot(value, up[...], preferred_element_type=jnp.float32)
        active = (opened / (1.0 + jnp.exp(-opened)) * upper).astype(jnp.bfloat16)
        return jnp.dot(active, down[...], preferred_element_type=jnp.float32).astype(jnp.bfloat16)

    def spots(notes, who):
        line = column(notes[pl.ds(who, 1), :])
        worth = column(notes[pl.ds(who + lines, 1), :])
        slot = lax.broadcasted_iota(jnp.int32, (tok_rows, capacity), 1)
        full = jnp.where(line == slot.astype(jnp.float32), worth, 0.0)
        coarse = full.astype(jnp.bfloat16)
        return coarse, (full - coarse.astype(jnp.float32)).astype(jnp.bfloat16)

    def spread(coarse, fine, value):
        return jnp.dot(coarse, value, preferred_element_type=jnp.float32) + jnp.dot(
            fine, value, preferred_element_type=jnp.float32
        )

    image = column(facts[2 * lines : 2 * lines + 1, :])
    rows = 64
    for start in range(0, tok_rows, rows):
        normalize_rows(tokens, normed, image, start, rows)

    def send(wave):
        packed[0, wave_rows(wave)] = pack(facts, normed, second, wave)
        go(0, wave).start()

    each(waves, send)

    for load in loads[4:]:
        load.wait()

    def local(wave):
        here = wave_rows(wave)
        own_results[here] = feed(pack(facts, normed, me, wave))

    each(waves, local)
    total[...] = tokens[...].astype(jnp.float32) + spread(*spots(facts, me), own_results[...])

    def serve(kind, now):
        def step(wave):
            here = wave_rows(wave)
            go(kind, wave).wait_recv()
            finished[kind, here] = feed(arrived[kind, here])

            @pl.when(wave < now)
            def _():
                back(kind, wave).start()

        each(waves, step)

    serve(0, waves - 1)

    told.wait_recv()
    near_image = column(near_facts[2 * lines : 2 * lines + 1, :])
    for block in range(blocks):
        dense(block).wait_recv()
        for start in range(block * part, (block + 1) * part, rows):
            normalize_rows(near_tokens, near_normed, near_image, start, rows)

    def forward(wave):
        packed[1, wave_rows(wave)] = pack(near_facts, near_normed, second, wave)
        go(1, wave).start()

    each(waves, forward)

    def near_local(wave):
        here = wave_rows(wave)
        own_rows[here] = feed(pack(near_facts, near_normed, me, wave))

    each(waves, near_local)
    near_total[...] = spread(*spots(near_facts, me), own_rows[...])

    serve(1, waves)
    back(0, waves - 1).start()

    coarse, fine = spots(near_facts, second)
    each(waves, lambda wave: back(1, wave).wait_recv())
    for block in range(blocks):
        here = slice(block * part, (block + 1) * part)
        sum_out[here, :] = (
            near_total[here, :] + spread(coarse[here], fine[here], returned[1])
        ).astype(jnp.bfloat16)
        sums(block).start()

    each(waves, lambda wave: back(0, wave).wait_recv())
    total[...] += spread(*spots(facts, second), returned[0])

    for block in range(blocks):
        here = slice(block * part, (block + 1) * part)
        sums(block).wait_recv()
        out_ref[here, :] = (total[here, :] + sum_in[here, :].astype(jnp.float32)).astype(
            out_ref.dtype
        )

    told.wait_send()
    each(blocks, lambda block: dense(block).wait_send())
    each(blocks, lambda block: sums(block).wait_send())
    for kind in range(2):
        each(waves, lambda wave: go(kind, wave).wait_send())
        each(waves, lambda wave: back(kind, wave).wait_send())


def relay_scratch(tok_rows, width, hidden, fanout, capacity, waves, blocks):
    dense = pltpu.VMEM((tok_rows, width), jnp.bfloat16)
    sums = pltpu.VMEM((tok_rows, width), jnp.float32)
    facts = pltpu.VMEM((24, tok_rows), jnp.float32)
    slots = pltpu.VMEM((2, capacity, width), jnp.bfloat16)
    single = pltpu.VMEM((capacity, width), jnp.bfloat16)
    wide = pltpu.VMEM((width, hidden), jnp.bfloat16)
    by_block = pltpu.SemaphoreType.DMA((blocks,))
    by_wave = pltpu.SemaphoreType.DMA((2, waves))
    return [
        pltpu.VMEM((1, tok_rows), jnp.int32), pltpu.VMEM((fanout, tok_rows), jnp.int32),
        pltpu.VMEM((fanout, tok_rows), jnp.float32), pltpu.VMEM((2, width), jnp.float32),
        dense, dense, wide, wide, pltpu.VMEM((hidden, width), jnp.bfloat16), dense, dense,
        sums, sums, facts, facts, slots, slots, slots, slots, single, single, dense, dense,
        pltpu.SemaphoreType.DMA((7,)), by_block, pltpu.SemaphoreType.DMA((2,)), by_block, by_block,
        by_wave, by_wave, by_wave, by_wave, by_block, by_block,
    ]


def direct_scratch(tok_rows, width, hidden, buffer, sems):
    return [
        pltpu.VMEM((tok_rows, width), jnp.bfloat16),
        pltpu.VMEM((width, hidden), jnp.bfloat16),
        pltpu.VMEM((width, hidden), jnp.bfloat16),
        pltpu.VMEM((hidden, width), jnp.bfloat16),
        pltpu.VMEM((tok_rows, width), jnp.bfloat16),
        pltpu.VMEM((tok_rows, width), jnp.float32),
        pltpu.VMEM((LANES, tok_rows), jnp.float32),
        pltpu.VMEM((tok_rows, LANES), jnp.float32),
        pltpu.VMEM((tok_rows, LANES), jnp.float32),
        buffer,
        buffer,
        buffer,
        buffer,
        pltpu.SemaphoreType.DMA((4,)),
        sems,
        sems,
        sems,
        sems,
    ]


def shards(
    tokens, modality, expert_ids, route_weights, norm_gain, gate_weight, up_weight, down_weight
):
    devices = lax.axis_size(AXIS)
    tok_rows, width = tokens.shape
    fanout = expert_ids.shape[1]
    hidden = gate_weight.shape[1]
    capacity = min(tok_rows, tok_rows * fanout * 5 // (4 * devices))
    waves = 2 if capacity % 32 == 0 and capacity >= 256 else 1
    chunk = capacity // waves
    buffer = pltpu.VMEM((waves, devices, chunk, width), jnp.bfloat16)
    near = pl.BlockSpec(memory_space=pltpu.VMEM)
    far = pl.BlockSpec(memory_space=pl.ANY)
    sems = pltpu.SemaphoreType.DMA((waves, devices))
    blocks = 4
    relayed = devices == 4 and tok_rows % (64 * blocks) == 0 and capacity % 32 == 0
    if relayed:
        kernel = functools.partial(relay_kernel, blocks)
        scratch = relay_scratch(tok_rows, width, hidden, fanout, capacity, 2, blocks)
    else:
        kernel = functools.partial(moe_kernel, devices)
        scratch = direct_scratch(tok_rows, width, hidden, buffer, sems)
    return pl.pallas_call(
        kernel,
        out_shape=pltpu.VMEM((tok_rows, width), jnp.bfloat16),
        in_specs=[far] + [far if relayed else near] * 4 + [far] * 3,
        out_specs=near,
        scratch_shapes=scratch,
        compiler_params=pltpu.CompilerParams(
            collective_id=0, has_side_effects=True, vmem_limit_bytes=58 * 1024 * 1024
        ),
    )(
        tokens,
        modality.reshape(1, tok_rows),
        expert_ids.T,
        route_weights.T,
        norm_gain,
        gate_weight,
        up_weight,
        down_weight,
    )


def solution(mesh):
    placed = (
        P(("dp", AXIS), None),
        P(("dp", AXIS)),
        P(("dp", AXIS), None),
        P(("dp", AXIS), None),
        P(),
        P(None, AXIS),
        P(None, AXIS),
        P(AXIS, None),
    )
    return jax.shard_map(
        shards, mesh=mesh, in_specs=placed, out_specs=P(("dp", AXIS), None), check_vma=False
    )
```

```python
import functools

import jax
import jax.numpy as jnp
from jax import lax
from jax.experimental import pallas as pl
from jax.experimental.pallas import tpu as pltpu
from jax.sharding import PartitionSpec as P

epsilon = 1e-05
LANES = 128
AXIS = "expert"


def grid_side(devices):
    side = 1
    while side * side < devices:
        side += 1
    return side if side * side == devices else devices


def moe_kernel(
    devices,
    tokens_hbm,
    modality_ref,
    ids_ref,
    weights_ref,
    gain_ref,
    gate_hbm,
    up_hbm,
    down_hbm,
    out_ref,
    tokens,
    gate,
    up,
    down,
    normed,
    total,
    place_rows,
    place_cols,
    share_cols,
    packed,
    arrived,
    finished,
    returned,
    load_sem,
    go_send,
    go_recv,
    back_send,
    back_recv,
):
    waves, _, chunk, width = packed.shape
    tok_rows = tokens.shape[0]
    fanout = ids_ref.shape[0]
    me = lax.axis_index(AXIS)
    side = grid_side(devices)
    mine_hi, mine_lo = me // side, me % side
    lines = devices // side

    def ahead(step):
        return ((mine_hi + step // side) % lines) * side + (mine_lo + step % side) % side

    def behind(step):
        return ((mine_hi + lines - step // side) % lines) * side + (
            mine_lo + side - step % side
        ) % side

    def go(wave, step):
        return pltpu.make_async_remote_copy(
            src_ref=packed.at[wave, step],
            dst_ref=arrived.at[wave, step],
            send_sem=go_send.at[wave, step],
            recv_sem=go_recv.at[wave, step],
            device_id={AXIS: ahead(step)},
            device_id_type=pl.DeviceIdType.MESH,
        )

    def back(wave, step):
        return pltpu.make_async_remote_copy(
            src_ref=finished.at[wave, step],
            dst_ref=returned.at[wave, step],
            send_sem=back_send.at[wave, step],
            recv_sem=back_recv.at[wave, step],
            device_id={AXIS: behind(step)},
            device_id_type=pl.DeviceIdType.MESH,
        )

    loads = [
        pltpu.make_async_copy(tokens_hbm, tokens, load_sem.at[0]),
        pltpu.make_async_copy(gate_hbm, gate, load_sem.at[1]),
        pltpu.make_async_copy(up_hbm, up, load_sem.at[2]),
        pltpu.make_async_copy(down_hbm, down, load_sem.at[3]),
    ]
    for load in loads:
        load.start()

    barrier = pltpu.get_barrier_semaphore()

    def greet(step, carry):
        pl.semaphore_signal(
            barrier, inc=1, device_id={AXIS: ahead(step)}, device_id_type=pl.DeviceIdType.MESH
        )
        return carry

    lax.fori_loop(1, devices, greet, 0)

    expert = lax.broadcasted_iota(jnp.int32, (LANES, tok_rows), 0)
    named = jnp.zeros((LANES, tok_rows), jnp.float32)
    share = jnp.zeros((LANES, tok_rows), jnp.float32)
    for k in range(fanout):
        hit = expert == ids_ref[k : k + 1, :]
        named = jnp.where(hit, 1.0, named)
        share = jnp.where(hit, weights_ref[k : k + 1, :], share)
    before = (
        lax.broadcasted_iota(jnp.int32, (tok_rows, tok_rows), 0)
        < lax.broadcasted_iota(jnp.int32, (tok_rows, tok_rows), 1)
    )
    count = jnp.dot(
        named.astype(jnp.bfloat16),
        jnp.where(before, 1.0, 0.0).astype(jnp.bfloat16),
        preferred_element_type=jnp.float32,
    )
    place = jnp.where(named > 0.5, count, -1.0)
    place_rows[...] = place
    place_cols[...] = place.T
    share_cols[...] = share.T
    image = jnp.broadcast_to(modality_ref[...].astype(jnp.float32), (LANES, tok_rows)).T

    loads[0].wait()
    rows = 64
    for start in range(0, tok_rows, rows):
        values = tokens[start : start + rows, :].astype(jnp.float32)
        square = jnp.mean(values * values, axis=1, keepdims=True)
        gains = jnp.where(
            image[start : start + rows, :1] > 0.5, gain_ref[1:2, :], gain_ref[0:1, :]
        )
        normed[start : start + rows, :] = (
            values * lax.rsqrt(square + epsilon) * gains
        ).astype(jnp.bfloat16)

    def pack(wave, step, target):
        line = place_rows[pl.ds(ahead(step), 1), :]
        slot = lax.broadcasted_iota(jnp.int32, (chunk, tok_rows), 0) + wave * chunk
        pick = jnp.where(line == slot.astype(jnp.float32), 1.0, 0.0).astype(jnp.bfloat16)
        target[wave, step] = jnp.dot(
            pick, normed[...], preferred_element_type=jnp.float32
        ).astype(jnp.bfloat16)

    others = devices - 1
    items = waves * others

    def which(item):
        return item // others, others - item % others

    pl.semaphore_wait(barrier, others)

    def send(item, carry):
        wave, step = which(item)
        pack(wave, step, packed)
        go(wave, step).start()
        return carry

    lax.fori_loop(0, items, send, 0)

    for load in loads[1:]:
        load.wait()

    def feed(source, target, wave, step):
        value = source[wave, step]
        opened = jnp.dot(value, gate[...], preferred_element_type=jnp.float32)
        upper = jnp.dot(value, up[...], preferred_element_type=jnp.float32)
        active = (opened / (1.0 + jnp.exp(-opened)) * upper).astype(jnp.bfloat16)
        target[wave, step] = jnp.dot(
            active, down[...], preferred_element_type=jnp.float32
        ).astype(jnp.bfloat16)

    def spread(wave, step):
        lane = lax.broadcasted_iota(jnp.int32, (tok_rows, LANES), 1) == ahead(step)
        line = jnp.sum(jnp.where(lane, place_cols[...], 0.0), axis=1, keepdims=True)
        worth = jnp.sum(jnp.where(lane, share_cols[...], 0.0), axis=1, keepdims=True)
        slot = lax.broadcasted_iota(jnp.int32, (tok_rows, chunk), 1) + wave * chunk
        spots = jnp.where(line == slot.astype(jnp.float32), worth, 0.0)
        high = spots.astype(jnp.bfloat16)
        low = (spots - high.astype(jnp.float32)).astype(jnp.bfloat16)
        value = returned[wave, step]
        return jnp.dot(high, value, preferred_element_type=jnp.float32) + jnp.dot(
            low, value, preferred_element_type=jnp.float32
        )

    total[...] = tokens[...].astype(jnp.float32)

    def local(wave, carry):
        pack(wave, 0, arrived)
        feed(arrived, returned, wave, 0)
        total[...] += spread(wave, 0)
        return carry

    lax.fori_loop(0, waves, local, 0)

    def serve(item, carry):
        wave, step = which(item)
        go(wave, step).wait_recv()
        feed(arrived, finished, wave, step)
        back(wave, step).start()
        return carry

    lax.fori_loop(0, items, serve, 0)

    def collect(item, carry):
        wave, step = which(item)
        back(wave, step).wait_recv()
        total[...] += spread(wave, step)
        return carry

    lax.fori_loop(0, items - 1, collect, 0)
    wave, step = which(items - 1)
    back(wave, step).wait_recv()
    out_ref[...] = (total[...] + spread(wave, step)).astype(out_ref.dtype)

    def settle(item, carry):
        wave, step = which(item)
        go(wave, step).wait_send()
        back(wave, step).wait_send()
        return carry

    lax.fori_loop(0, items, settle, 0)


def relay_kernel(
    blocks,
    tokens_hbm,
    modality_hbm,
    ids_hbm,
    weights_hbm,
    gain_hbm,
    gate_hbm,
    up_hbm,
    down_hbm,
    out_ref,
    modality_ref,
    ids_ref,
    weights_ref,
    gain_ref,
    tokens,
    near_tokens,
    gate,
    up,
    down,
    normed,
    near_normed,
    total,
    near_total,
    facts,
    near_facts,
    packed,
    arrived,
    finished,
    returned,
    own_rows,
    own_results,
    sum_out,
    sum_in,
    load_sem,
    token_sem,
    facts_sem,
    dense_send,
    dense_recv,
    go_send,
    go_recv,
    back_send,
    back_recv,
    sum_send,
    sum_recv,
):
    _, capacity, width = packed.shape
    waves = go_send.shape[1]
    chunk = capacity // waves
    tok_rows = tokens.shape[0]
    part = tok_rows // blocks
    fanout = ids_ref.shape[0]
    me = lax.axis_index(AXIS)
    role = lax.axis_index("dp") % 2
    high, low = me // 2, me % 2
    beside = high * 2 + 1 - low
    above = (1 - high) * 2 + low
    first = beside * (1 - role) + above * role
    second = above * (1 - role) + beside * role

    def remote(source, target, send_sem, recv_sem, peer):
        return pltpu.make_async_remote_copy(
            src_ref=source,
            dst_ref=target,
            send_sem=send_sem,
            recv_sem=recv_sem,
            device_id={AXIS: peer},
            device_id_type=pl.DeviceIdType.MESH,
        )

    def part_rows(block):
        return pl.ds(pl.multiple_of(block * part, part), part)

    def wave_rows(wave):
        if isinstance(wave, int):
            return slice(wave * chunk, (wave + 1) * chunk)
        return pl.ds(pl.multiple_of(wave * chunk, chunk), chunk)

    def dense(block):
        rows = part_rows(block)
        return remote(
            tokens.at[rows], near_tokens.at[rows], dense_send.at[block], dense_recv.at[block], first
        )

    def go(kind, wave):
        rows = wave_rows(wave)
        return remote(
            packed.at[kind, rows],
            arrived.at[kind, rows],
            go_send.at[kind, wave],
            go_recv.at[kind, wave],
            second,
        )

    def back(kind, wave):
        rows = wave_rows(wave)
        return remote(
            finished.at[kind, rows],
            returned.at[kind, rows],
            back_send.at[kind, wave],
            back_recv.at[kind, wave],
            second,
        )

    def sums(block):
        rows = part_rows(block)
        return remote(
            sum_out.at[rows], sum_in.at[rows], sum_send.at[block], sum_recv.at[block], first
        )

    def each(count, step):
        def body(index, carry):
            step(index)
            return carry

        lax.fori_loop(0, count, body, 0)

    loads = [
        pltpu.make_async_copy(source, target, load_sem.at[index])
        for index, (source, target) in enumerate(
            (
                (ids_hbm, ids_ref),
                (weights_hbm, weights_ref),
                (modality_hbm, modality_ref),
                (gain_hbm, gain_ref),
                (gate_hbm, gate),
                (up_hbm, up),
                (down_hbm, down),
            )
        )
    ]

    def token_load(block):
        rows = part_rows(block)
        return pltpu.make_async_copy(tokens_hbm.at[rows], tokens.at[rows], token_sem.at[block])

    each(blocks, lambda block: token_load(block).start())
    for load in loads[:4]:
        load.start()
    barrier = pltpu.get_barrier_semaphore()
    for peer in (first, second):
        pl.semaphore_signal(
            barrier, inc=1, device_id={AXIS: peer}, device_id_type=pl.DeviceIdType.MESH
        )
    pl.semaphore_wait(barrier, 2)

    def leave(block):
        token_load(block).wait()
        dense(block).start()

    each(blocks, leave)
    for load in loads[4:]:
        load.start()
    for load in loads[:4]:
        load.wait()

    lines = 8
    expert = lax.broadcasted_iota(jnp.int32, (lines, tok_rows), 0)
    named = jnp.zeros((lines, tok_rows), jnp.float32)
    share = jnp.zeros((lines, tok_rows), jnp.float32)
    for k in range(fanout):
        hit = expert == ids_ref[k : k + 1, :]
        named = jnp.where(hit, 1.0, named)
        share = jnp.where(hit, weights_ref[k : k + 1, :], share)
    before = (
        lax.broadcasted_iota(jnp.int32, (tok_rows, tok_rows), 0)
        < lax.broadcasted_iota(jnp.int32, (tok_rows, tok_rows), 1)
    )
    count = jnp.dot(
        named.astype(jnp.bfloat16),
        jnp.where(before, 1.0, 0.0).astype(jnp.bfloat16),
        preferred_element_type=jnp.float32,
    )
    facts[0:lines, :] = jnp.where(named > 0.5, count, -1.0)
    facts[lines : 2 * lines, :] = share
    facts[2 * lines : 3 * lines, :] = jnp.broadcast_to(
        modality_ref[...].astype(jnp.float32), (lines, tok_rows)
    )
    told = remote(facts, near_facts, facts_sem.at[0], facts_sem.at[1], first)
    told.start()

    def column(line):
        return jnp.broadcast_to(line, (LANES, tok_rows)).T[:, :1]

    def normalize_rows(source, target, image, start, rows):
        values = source[start : start + rows, :].astype(jnp.float32)
        square = jnp.mean(values * values, axis=1, keepdims=True)
        gains = jnp.where(
            image[start : start + rows] > 0.5, gain_ref[1:2, :], gain_ref[0:1, :]
        )
        target[start : start + rows, :] = (
            values * lax.rsqrt(square + epsilon) * gains
        ).astype(jnp.bfloat16)

    def pack(notes, rows, who, wave):
        line = notes[pl.ds(who, 1), :]
        slot = lax.broadcasted_iota(jnp.int32, (chunk, tok_rows), 0) + wave * chunk
        pick = jnp.where(line == slot.astype(jnp.float32), 1.0, 0.0).astype(jnp.bfloat16)
        return jnp.dot(pick, rows[...], preferred_element_type=jnp.float32).astype(jnp.bfloat16)

    def feed(value):
        opened = jnp.dot(value, gate[...], preferred_element_type=jnp.float32)
        upper = jnp.dot(value, up[...], preferred_element_type=jnp.float32)
        active = (opened / (1.0 + jnp.exp(-opened)) * upper).astype(jnp.bfloat16)
        return jnp.dot(active, down[...], preferred_element_type=jnp.float32).astype(jnp.bfloat16)

    def spots(notes, who):
        line = column(notes[pl.ds(who, 1), :])
        worth = column(notes[pl.ds(who + lines, 1), :])
        slot = lax.broadcasted_iota(jnp.int32, (tok_rows, capacity), 1)
        full = jnp.where(line == slot.astype(jnp.float32), worth, 0.0)
        coarse = full.astype(jnp.bfloat16)
        return coarse, (full - coarse.astype(jnp.float32)).astype(jnp.bfloat16)

    def spread(coarse, fine, value):
        return jnp.dot(coarse, value, preferred_element_type=jnp.float32) + jnp.dot(
            fine, value, preferred_element_type=jnp.float32
        )

    image = column(facts[2 * lines : 2 * lines + 1, :])
    rows = 64
    for start in range(0, tok_rows, rows):
        normalize_rows(tokens, normed, image, start, rows)

    def send(wave):
        packed[0, wave_rows(wave)] = pack(facts, normed, second, wave)
        go(0, wave).start()

    each(waves, send)

    for load in loads[4:]:
        load.wait()

    def local(wave):
        here = wave_rows(wave)
        own_results[here] = feed(pack(facts, normed, me, wave))

    each(waves, local)
    total[...] = tokens[...].astype(jnp.float32) + spread(*spots(facts, me), own_results[...])

    def serve(kind, now):
        def step(wave):
            here = wave_rows(wave)
            go(kind, wave).wait_recv()
            finished[kind, here] = feed(arrived[kind, here])

            @pl.when(wave < now)
            def _():
                back(kind, wave).start()

        each(waves, step)

    serve(0, waves - 1)

    told.wait_recv()
    near_image = column(near_facts[2 * lines : 2 * lines + 1, :])
    for block in range(blocks):
        dense(block).wait_recv()
        for start in range(block * part, (block + 1) * part, rows):
            normalize_rows(near_tokens, near_normed, near_image, start, rows)

    def forward(wave):
        packed[1, wave_rows(wave)] = pack(near_facts, near_normed, second, wave)
        go(1, wave).start()

    each(waves, forward)

    def near_local(wave):
        here = wave_rows(wave)
        own_rows[here] = feed(pack(near_facts, near_normed, me, wave))

    near_local(0)

    serve(1, waves)
    back(0, waves - 1).start()

    for wave in range(1, waves):
        near_local(wave)
    near_total[...] = spread(*spots(near_facts, me), own_rows[...])

    coarse, fine = spots(near_facts, second)
    each(waves, lambda wave: back(1, wave).wait_recv())
    for block in range(blocks):
        here = slice(block * part, (block + 1) * part)
        sum_out[here, :] = (
            near_total[here, :] + spread(coarse[here], fine[here], returned[1])
        ).astype(jnp.bfloat16)
        sums(block).start()

    each(waves, lambda wave: back(0, wave).wait_recv())
    total[...] += spread(*spots(facts, second), returned[0])

    for block in range(blocks):
        here = slice(block * part, (block + 1) * part)
        sums(block).wait_recv()
        out_ref[here, :] = (total[here, :] + sum_in[here, :].astype(jnp.float32)).astype(
            out_ref.dtype
        )

    told.wait_send()
    each(blocks, lambda block: dense(block).wait_send())
    each(blocks, lambda block: sums(block).wait_send())
    for kind in range(2):
        each(waves, lambda wave: go(kind, wave).wait_send())
        each(waves, lambda wave: back(kind, wave).wait_send())


def relay_scratch(tok_rows, width, hidden, fanout, capacity, waves, blocks):
    dense = pltpu.VMEM((tok_rows, width), jnp.bfloat16)
    sums = pltpu.VMEM((tok_rows, width), jnp.float32)
    facts = pltpu.VMEM((24, tok_rows), jnp.float32)
    slots = pltpu.VMEM((2, capacity, width), jnp.bfloat16)
    single = pltpu.VMEM((capacity, width), jnp.bfloat16)
    wide = pltpu.VMEM((width, hidden), jnp.bfloat16)
    by_block = pltpu.SemaphoreType.DMA((blocks,))
    by_wave = pltpu.SemaphoreType.DMA((2, waves))
    return [
        pltpu.VMEM((1, tok_rows), jnp.int32), pltpu.VMEM((fanout, tok_rows), jnp.int32),
        pltpu.VMEM((fanout, tok_rows), jnp.float32), pltpu.VMEM((2, width), jnp.float32),
        dense, dense, wide, wide, pltpu.VMEM((hidden, width), jnp.bfloat16), dense, dense,
        sums, sums, facts, facts, slots, slots, slots, slots, single, single, dense, dense,
        pltpu.SemaphoreType.DMA((7,)), by_block, pltpu.SemaphoreType.DMA((2,)), by_block, by_block,
        by_wave, by_wave, by_wave, by_wave, by_block, by_block,
    ]


def direct_scratch(tok_rows, width, hidden, buffer, sems):
    return [
        pltpu.VMEM((tok_rows, width), jnp.bfloat16),
        pltpu.VMEM((width, hidden), jnp.bfloat16),
        pltpu.VMEM((width, hidden), jnp.bfloat16),
        pltpu.VMEM((hidden, width), jnp.bfloat16),
        pltpu.VMEM((tok_rows, width), jnp.bfloat16),
        pltpu.VMEM((tok_rows, width), jnp.float32),
        pltpu.VMEM((LANES, tok_rows), jnp.float32),
        pltpu.VMEM((tok_rows, LANES), jnp.float32),
        pltpu.VMEM((tok_rows, LANES), jnp.float32),
        buffer,
        buffer,
        buffer,
        buffer,
        pltpu.SemaphoreType.DMA((4,)),
        sems,
        sems,
        sems,
        sems,
    ]


def shards(
    tokens, modality, expert_ids, route_weights, norm_gain, gate_weight, up_weight, down_weight
):
    devices = lax.axis_size(AXIS)
    tok_rows, width = tokens.shape
    fanout = expert_ids.shape[1]
    hidden = gate_weight.shape[1]
    capacity = min(tok_rows, tok_rows * fanout * 5 // (4 * devices))
    waves = 2 if capacity % 32 == 0 and capacity >= 256 else 1
    chunk = capacity // waves
    buffer = pltpu.VMEM((waves, devices, chunk, width), jnp.bfloat16)
    near = pl.BlockSpec(memory_space=pltpu.VMEM)
    far = pl.BlockSpec(memory_space=pl.ANY)
    sems = pltpu.SemaphoreType.DMA((waves, devices))
    blocks = 4
    relayed = devices == 4 and tok_rows % (64 * blocks) == 0 and capacity % 32 == 0
    if relayed:
        kernel = functools.partial(relay_kernel, blocks)
        scratch = relay_scratch(tok_rows, width, hidden, fanout, capacity, 2, blocks)
    else:
        kernel = functools.partial(moe_kernel, devices)
        scratch = direct_scratch(tok_rows, width, hidden, buffer, sems)
    return pl.pallas_call(
        kernel,
        out_shape=pltpu.VMEM((tok_rows, width), jnp.bfloat16),
        in_specs=[far] + [far if relayed else near] * 4 + [far] * 3,
        out_specs=near,
        scratch_shapes=scratch,
        compiler_params=pltpu.CompilerParams(
            collective_id=0, has_side_effects=True, vmem_limit_bytes=58 * 1024 * 1024
        ),
    )(
        tokens,
        modality.reshape(1, tok_rows),
        expert_ids.T,
        route_weights.T,
        norm_gain,
        gate_weight,
        up_weight,
        down_weight,
    )


def solution(mesh):
    placed = (
        P(("dp", AXIS), None),
        P(("dp", AXIS)),
        P(("dp", AXIS), None),
        P(("dp", AXIS), None),
        P(),
        P(None, AXIS),
        P(None, AXIS),
        P(AXIS, None),
    )
    return jax.shard_map(
        shards, mesh=mesh, in_specs=placed, out_specs=P(("dp", AXIS), None), check_vma=False
    )
```
